256 devices in a mesh: row: 16 (over z, core), col: 16 (over y, x).
Axes of the slice: x: 4, y: 4, z: 8, core: 2. Of those that a mesh axis runs over, the one named last changes fastest.
Arguments:
- factor: float32 [10240, 10240], P('row', 'col'), may hold values from -1 to 6, as said below
Outputs:
- progressed: float32 [10240, 10240], P('row', 'col')
The draws below stay inside these ranges and needn't reach their ends.
Inputs may be any that keep to these rules, and one draw needn't show every extreme that they name: factor is symmetric positive definite with smallest eigenvalue at least 0.5, stored in the block-cyclic order of the steps.
All inputs are finite; a program needn't handle non-finite values.
Results may differ from the reference program's by a relative error of at most 0.0001.
Values sent between devices are 32-bit elements; how exact they have to be, the bound alone decides.
No kernel may reach another device: no remote copies, remote signals or barrier semaphores. Data moves between devices by JAX's collectives and lax.ppermute only.
A program may use at most 128 MiB of HBM per device.

```python
import jax
import jax.numpy as jnp
from jax import lax

N = 10240
TILE = 128
PIVOT = 512
STEPS = 2
N_ROW = 16
N_COL = 16


def draw_factor(key, part):
    normal_key, spread_key = jax.random.split(jax.random.fold_in(key, 11), 2)
    inner_width = 4 * PIVOT
    directions = jax.random.normal(normal_key, (N, inner_width), jnp.float32)
    weights = jnp.full((inner_width,), N / inner_width, jnp.float32)
    damping = jnp.exp(jax.random.uniform(spread_key, (N,), jnp.float32, jnp.log(0.5), jnp.log(2.0)))
    loadings = directions * jnp.sqrt(weights / N)[None, :]
    product = jnp.dot(loadings, loadings.T, precision=lax.Precision.HIGHEST, preferred_element_type=jnp.float32)
    logical = 0.5 * (product + product.T) + jnp.diag(damping)
    rows_tiles = N // (N_ROW * TILE)
    cols_tiles = N // (N_COL * TILE)
    moved = logical.reshape(rows_tiles, N_ROW, TILE, N).transpose(1, 0, 2, 3).reshape(N, N)
    moved = moved.reshape(N, cols_tiles, N_COL, TILE).transpose(0, 2, 1, 3).reshape(N, N)
    return moved.astype(jnp.float32)


def setup_inputs(seed: int = 0) -> dict:
    seeds = jax.random.split(jax.random.key(seed), 2)
    factor = draw_factor(jax.random.fold_in(seeds[1], 71), 0)
    return dict(factor=factor)


def to_logical(stored):
    rows_tiles = N // (N_ROW * TILE)
    cols_tiles = N // (N_COL * TILE)
    moved = stored.reshape(N_ROW, rows_tiles, TILE, N).transpose(1, 0, 2, 3).reshape(N, N)
    moved = moved.reshape(N, N_COL, cols_tiles, TILE).transpose(0, 2, 1, 3).reshape(N, N)
    return moved

def to_stored(logical):
    rows_tiles = N // (N_ROW * TILE)
    cols_tiles = N // (N_COL * TILE)
    moved = logical.reshape(rows_tiles, N_ROW, TILE, N).transpose(1, 0, 2, 3).reshape(N, N)
    moved = moved.reshape(N, cols_tiles, N_COL, TILE).transpose(0, 2, 1, 3).reshape(N, N)
    return moved

def reference(factor):
    matrix = to_logical(factor)
    identity = jnp.eye(PIVOT, dtype=jnp.float32)
    for step in range(STEPS):
        start = step * PIVOT
        pivot_block = matrix[start:start + PIVOT, start:start + PIVOT]
        lower = jnp.linalg.cholesky(pivot_block)
        inverse = jax.scipy.linalg.cho_solve((lower, True), identity)
        scaled = jnp.dot(inverse.astype(jnp.float32), matrix[start:start + PIVOT, :].astype(jnp.float32), precision=lax.Precision.HIGHEST, preferred_element_type=jnp.float32)
        marks = jnp.zeros((N, PIVOT), jnp.float32).at[start:start + PIVOT, :].set(identity)
        reduced = matrix[:, start:start + PIVOT] - marks
        matrix = matrix - jnp.dot(reduced.astype(jnp.float32), scaled.astype(jnp.float32), precision=lax.Precision.HIGHEST, preferred_element_type=jnp.float32)
        fixed = marks - jnp.dot(reduced.astype(jnp.float32), inverse.astype(jnp.float32), precision=lax.Precision.HIGHEST, preferred_element_type=jnp.float32)
        matrix = matrix.at[:, start:start + PIVOT].set(fixed)
    return to_stored(matrix)
```

```python
import jax
import jax.numpy as jnp
from jax import lax
from jax.experimental import pallas as pl
from jax.experimental.pallas import tpu as pltpu
from jax.sharding import PartitionSpec as P

TILE = 128
PIVOT = 512
STEPS = 2
K = PIVOT * STEPS
KT = K // TILE
HI = lax.Precision.HIGHEST
NZ, NY, NX = 8, 4, 4


def dot(a, b):
    return jnp.dot(a, b, precision=HI, preferred_element_type=jnp.float32)


def spread(x, e):
    return jnp.broadcast_to(x[e : e + 1, :], x.shape)


def invert_tile(block, b=16):
    n = TILE
    nb = b // 8
    nt = n // 8
    a = [block[8 * t : 8 * t + 8, :] for t in range(nt)]
    lane = lax.broadcasted_iota(jnp.int32, (8, n), 1)
    row = lax.broadcasted_iota(jnp.int32, (8, n), 0)
    for s in range(n // b):
        base = b * s
        own = [nb * s + q for q in range(nb)]
        inside = (lane >= base) & (lane < base + b)

        def col(t, j):
            return jnp.broadcast_to(a[t][:, base + j : base + j + 1], (8, n))

        c = [[col(t, j) for t in own] for j in range(b)]
        rows = [a[t] for t in own]
        for i in range(0, b, 2):
            h, e = divmod(i, 8)
            p, q_, w, o_ = spread(c[i][h], e), spread(c[i + 1][h], e), spread(c[i + 1][h], e + 1), spread(c[i][h], e + 1)
            rd = 1.0 / (p * w - q_ * o_)
            r0, r1 = row == e, row == e + 1
            l0, l1 = lane == base + i, lane == base + i + 1
            for j in range(i + 2, b):
                x, y = spread(c[j][h], e), spread(c[j][h], e + 1)
                u = (w * x - q_ * y) * rd
                v = (p * y - o_ * x) * rd
                for q in range(nb):
                    new = c[j][q] - c[i][q] * u - c[i + 1][q] * v
                    c[j][q] = jnp.where(r0, u, jnp.where(r1, v, new)) if q == h else new
            x = jnp.where(l0, 1.0, jnp.where(l1, 0.0, spread(rows[h], e)))
            y = jnp.where(l0, 0.0, jnp.where(l1, 1.0, spread(rows[h], e + 1)))
            u = (w * x - q_ * y) * rd
            v = (p * y - o_ * x) * rd
            for q in range(nb):
                new = jnp.where(l0 | l1, 0.0, rows[q]) - c[i][q] * u - c[i + 1][q] * v
                rows[q] = jnp.where(r0, u, jnp.where(r1, v, new)) if q == h else new
        g = [spread(rows[i // 8], i % 8) for i in range(b)]
        nxt = [nb * (s + 1) + q for q in range(nb)] if s + 1 < n // b else []
        rest = [t for t in range(nt) if t not in own and t not in nxt]
        full = jnp.concatenate(a, axis=0)
        d = dot(full[:, base : base + b], jnp.concatenate(rows, axis=0))
        for t in nxt:
            acc = jnp.where(inside, 0.0, a[t])
            for i in range(b):
                acc = acc - col(t, i) * g[i]
            a[t] = acc
        for t in rest:
            a[t] = jnp.where(inside, 0.0, a[t]) - d[8 * t : 8 * t + 8, :]
        for q, t in enumerate(own):
            a[t] = rows[q]
    return jnp.concatenate(a, axis=0)


def split3(x):
    h = x.astype(jnp.bfloat16)
    r = x - h.astype(jnp.float32)
    m = r.astype(jnp.bfloat16)
    l = (r - m.astype(jnp.float32)).astype(jnp.bfloat16)
    return h, m, l


def bdot(a, b):
    return jnp.dot(a, b, preferred_element_type=jnp.float32)


def inverse_kernel(idx_ref, own_ref, oth_ref, a_ref, gh, gm, gl):
    q = idx_ref[0]
    x = idx_ref[1]
    for xs in range(NX):
        slot = lax.rem(x - xs + NX, NX)
        for ys in range(2):
            cols = slice((NX * ys + xs) * TILE, (NX * ys + xs + 1) * TILE)
            for s in range(KT // 2):
                mine = pl.ds(pl.multiple_of((2 * s + q) * TILE, TILE), TILE)
                other = pl.ds(pl.multiple_of((2 * s + 1 - q) * TILE, TILE), TILE)
                a_ref[mine, cols] = own_ref[slot, ys, s]
                a_ref[other, cols] = oth_ref[slot, ys, s]

    def step(k, carry):
        k0 = pl.multiple_of(k * 2 * TILE, 2 * TILE)
        d0, d1 = pl.ds(k0, TILE), pl.ds(pl.multiple_of(k0 + TILE, TILE), TILE)
        dd = pl.ds(k0, 2 * TILE)
        i0 = invert_tile(a_ref[d0, d0])
        b = a_ref[d0, d1]
        ct = a_ref[d1, d0]
        t = dot(i0, b)
        v = dot(ct, i0)
        i1 = invert_tile(a_ref[d1, d1] - dot(ct, t))
        ti = dot(t, i1)
        e = jnp.concatenate(
            [
                jnp.concatenate([i0 + dot(ti, v), -ti], axis=1),
                jnp.concatenate([-dot(i1, v), i1], axis=1),
            ],
            axis=0,
        )
        for half in range(2):
            cs = slice(half * K // 2, (half + 1) * K // 2)
            a_ref[dd, cs] = dot(e, a_ref[dd, cs])
        a_ref[dd, dd] = e
        h, m, l = split3(a_ref[dd, :])
        gh[...] = h
        gm[...] = m
        gl[...] = l

        def update(i, carry):
            @pl.when(lax.div(i, 2) != k)
            def _():
                ri = pl.ds(pl.multiple_of(i * TILE, TILE), TILE)
                lh, lm, ll = split3(a_ref[ri, dd])
                a_ref[ri, dd] = jnp.zeros((TILE, 2 * TILE), jnp.float32)
                for part in range(4):
                    cs = slice(part * K // 4, (part + 1) * K // 4)
                    low = bdot(lm, gm[:, cs]) + bdot(lh, gl[:, cs]) + bdot(ll, gh[:, cs])
                    mid = bdot(lh, gm[:, cs]) + bdot(lm, gh[:, cs])
                    a_ref[ri, cs] = a_ref[ri, cs] - (bdot(lh, gh[:, cs]) + (mid + low))

            return carry

        return lax.fori_loop(0, KT, update, carry)

    lax.fori_loop(0, K // (2 * TILE), step, 0)


def pivot_inverse(idx, own, oth):
    return pl.pallas_call(
        inverse_kernel,
        out_shape=jax.ShapeDtypeStruct((K, K), jnp.float32),
        in_specs=[
            pl.BlockSpec(memory_space=pltpu.SMEM),
            pl.BlockSpec(memory_space=pltpu.VMEM),
            pl.BlockSpec(memory_space=pltpu.VMEM),
        ],
        out_specs=pl.BlockSpec(memory_space=pltpu.VMEM),
        scratch_shapes=[pltpu.VMEM((2 * TILE, K), jnp.bfloat16)] * 3,
        name="pivot_inverse",
    )(idx, own, oth)


def z_pairs(d):
    return [(r, (r // 2 + d) % NZ * 2 + r % 2) for r in range(2 * NZ)]


def y_pairs(d):
    return [(c, (c // NX + d) % NY * NX + c % NX) for c in range(NX * NY)]


def x_pairs(d):
    return [(c, c // NX * NX + (c % NX + d) % NX) for c in range(NX * NY)]


FLIP = [(r, r ^ 1) for r in range(2 * NZ)]


def z_stage(v, z):
    up, down = [v], [v]
    for _ in range(4):
        up.append(lax.ppermute(up[-1], "row", z_pairs(1)))
    for _ in range(3):
        down.append(lax.ppermute(down[-1], "row", z_pairs(-1)))
    slots = up + down[:0:-1]
    return jnp.stack([lax.select_n(lax.rem(z - s + NZ, NZ), *slots) for s in range(4)])


def y_stage(v, y):
    up1 = lax.ppermute(v, "col", y_pairs(1))
    down1 = lax.ppermute(v, "col", y_pairs(-1))
    up2 = lax.ppermute(up1, "col", y_pairs(1))
    slots = [v, up1, up2, down1]
    return [lax.select_n(lax.rem(y - s + NY, NY), *slots) for s in range(2)]


def x_stage(pair):
    both = jnp.stack(pair)
    up1 = lax.ppermute(both, "col", x_pairs(1))
    down1 = lax.ppermute(both, "col", x_pairs(-1))
    far0 = lax.ppermute(up1[0], "col", x_pairs(1))
    far1 = lax.ppermute(down1[1], "col", x_pairs(-1))
    return jnp.stack([both, up1, jnp.stack([far0, far1]), down1])


def per_device(factor):
    row_place = lax.axis_index("row")
    col_place = lax.axis_index("col")
    z, q = row_place // 2, row_place % 2
    y, x = col_place // NX, col_place % NX

    corner = z_stage(factor[:TILE, :TILE], z)
    own = x_stage(y_stage(corner, y))
    other = lax.ppermute(own, "row", FLIP)

    panel = x_stage(y_stage(factor[:, :TILE], y))
    rest = z_stage(factor[:TILE, TILE:], z)
    mine = jnp.concatenate([corner, rest], axis=2)
    theirs = lax.ppermute(mine, "row", FLIP)

    idx = jnp.stack([q, x]).astype(jnp.int32)
    inverse = pivot_inverse(idx, own, other)

    even = jnp.where(q == 0, mine, theirs)
    odd = jnp.where(q == 0, theirs, mine)
    rows = jnp.stack([even, odd], axis=1).reshape(K, factor.shape[1])
    tiles = []
    for c in range(KT):
        tiles.append(lax.dynamic_index_in_dim(panel, lax.rem(x - c % NX + NX, NX), 0, keepdims=False)[c // NX])
    cols = jnp.concatenate(tiles, axis=1)

    is_pivot_col = (col_place < KT) & (jnp.arange(factor.shape[1]) < TILE)
    unit = jnp.arange(K)[:, None] == col_place * TILE + jnp.arange(factor.shape[1])[None, :]
    rows = jnp.where(is_pivot_col[None, :], unit.astype(jnp.float32), rows)
    base = jnp.where(is_pivot_col[None, :], 0.0, factor)

    scaled = dot(inverse, rows)
    updated = base - dot(cols, scaled)
    at = jnp.minimum(row_place, KT - 1) * TILE
    pivot_rows = lax.dynamic_slice(scaled, (at, 0), (TILE, factor.shape[1]))
    top = jnp.where(row_place < KT, pivot_rows, updated[:TILE])
    return lax.dynamic_update_slice(updated, top, (0, 0))


def solution(mesh):
    placed = (P("row", "col"),)
    return jax.shard_map(per_device, mesh=mesh, in_specs=placed, out_specs=P("row", "col"), check_vma=False)
```

```python
import jax
import jax.numpy as jnp
from jax import lax
from jax.experimental import pallas as pl
from jax.experimental.pallas import tpu as pltpu
from jax.sharding import PartitionSpec as P

TILE = 128
PIVOT = 512
STEPS = 2
K = PIVOT * STEPS
KT = K // TILE
HI = lax.Precision.HIGHEST
NZ, NY, NX = 8, 4, 4


def dot(a, b):
    return jnp.dot(a, b, precision=HI, preferred_element_type=jnp.float32)


def spread(x, e):
    return jnp.broadcast_to(x[e : e + 1, :], x.shape)


def invert_tile(block, b=16):
    n = TILE
    nb = b // 8
    nt = n // 8
    a = [block[8 * t : 8 * t + 8, :] for t in range(nt)]
    lane = lax.broadcasted_iota(jnp.int32, (8, n), 1)
    row = lax.broadcasted_iota(jnp.int32, (8, n), 0)
    for s in range(n // b):
        base = b * s
        own = [nb * s + q for q in range(nb)]
        inside = (lane >= base) & (lane < base + b)

        def col(t, j):
            return jnp.broadcast_to(a[t][:, base + j : base + j + 1], (8, n))

        c = [[col(t, j) for t in own] for j in range(b)]
        rows = [a[t] for t in own]
        for i in range(0, b, 2):
            h, e = divmod(i, 8)
            p, q_, w, o_ = spread(c[i][h], e), spread(c[i + 1][h], e), spread(c[i + 1][h], e + 1), spread(c[i][h], e + 1)
            rd = 1.0 / (p * w - q_ * o_)
            r0, r1 = row == e, row == e + 1
            l0, l1 = lane == base + i, lane == base + i + 1
            for j in range(i + 2, b):
                x, y = spread(c[j][h], e), spread(c[j][h], e + 1)
                u = (w * x - q_ * y) * rd
                v = (p * y - o_ * x) * rd
                for q in range(nb):
                    new = c[j][q] - c[i][q] * u - c[i + 1][q] * v
                    c[j][q] = jnp.where(r0, u, jnp.where(r1, v, new)) if q == h else new
            x = jnp.where(l0, 1.0, jnp.where(l1, 0.0, spread(rows[h], e)))
            y = jnp.where(l0, 0.0, jnp.where(l1, 1.0, spread(rows[h], e + 1)))
            u = (w * x - q_ * y) * rd
            v = (p * y - o_ * x) * rd
            for q in range(nb):
                new = jnp.where(l0 | l1, 0.0, rows[q]) - c[i][q] * u - c[i + 1][q] * v
                rows[q] = jnp.where(r0, u, jnp.where(r1, v, new)) if q == h else new
        g = [spread(rows[i // 8], i % 8) for i in range(b)]
        nxt = [nb * (s + 1) + q for q in range(nb)] if s + 1 < n // b else []
        rest = [t for t in range(nt) if t not in own and t not in nxt]
        full = jnp.concatenate(a, axis=0)
        d = dot(full[:, base : base + b], jnp.concatenate(rows, axis=0))
        for t in nxt:
            acc = jnp.where(inside, 0.0, a[t])
            for i in range(b):
                acc = acc - col(t, i) * g[i]
            a[t] = acc
        for t in rest:
            a[t] = jnp.where(inside, 0.0, a[t]) - d[8 * t : 8 * t + 8, :]
        for q, t in enumerate(own):
            a[t] = rows[q]
    return jnp.concatenate(a, axis=0)


def split3(x):
    h = x.astype(jnp.bfloat16)
    r = x - h.astype(jnp.float32)
    m = r.astype(jnp.bfloat16)
    l = (r - m.astype(jnp.float32)).astype(jnp.bfloat16)
    return h, m, l


def bdot(a, b):
    return jnp.dot(a, b, preferred_element_type=jnp.float32)


def six(l, r):
    low = bdot(l[1], r[1]) + bdot(l[0], r[2]) + bdot(l[2], r[0])
    return bdot(l[0], r[0]) + (bdot(l[0], r[1]) + bdot(l[1], r[0]) + low)


def schur_kernel(idx_ref, own_ref, oth_ref, mine_ref, theirs_ref, panel_ref, factor_ref, out_ref, m_ref, gh, gm, gl):
    q, x, r, c = idx_ref[0], idx_ref[1], idx_ref[2], idx_ref[3]
    size = factor_ref.shape[0]
    border = slice(K, K + size)
    for xs in range(NX):
        slot = lax.rem(x - xs + NX, NX)
        for ys in range(2):
            cols = slice((NX * ys + xs) * TILE, (NX * ys + xs + 1) * TILE)
            for s in range(KT // 2):
                mine = pl.ds(pl.multiple_of((2 * s + q) * TILE, TILE), TILE)
                other = pl.ds(pl.multiple_of((2 * s + 1 - q) * TILE, TILE), TILE)
                m_ref[mine, cols] = own_ref[slot, ys, s]
                m_ref[other, cols] = oth_ref[slot, ys, s]
            m_ref[border, cols] = panel_ref[slot, ys]
    for s in range(KT // 2):
        mine = pl.ds(pl.multiple_of((2 * s + q) * TILE, TILE), TILE)
        other = pl.ds(pl.multiple_of((2 * s + 1 - q) * TILE, TILE), TILE)
        m_ref[mine, border] = mine_ref[s]
        m_ref[other, border] = theirs_ref[s]
    m_ref[border, border] = factor_ref[...]
    first = slice(K, K + TILE)
    eye = (
        lax.broadcasted_iota(jnp.int32, (TILE, TILE), 0) == lax.broadcasted_iota(jnp.int32, (TILE, TILE), 1)
    ).astype(jnp.float32)

    @pl.when(c < KT)
    def _():
        m_ref[:, first] = jnp.zeros((K + size, TILE), jnp.float32)
        m_ref[pl.ds(pl.multiple_of(c * TILE, TILE), TILE), first] = eye

    @pl.when(r < KT)
    def _():
        m_ref[first, :] = jnp.where(
            lax.broadcasted_iota(jnp.int32, (TILE, K + size), 1)
            == lax.broadcasted_iota(jnp.int32, (TILE, K + size), 0) + r * TILE,
            -1.0,
            0.0,
        )

    wide = 2 * TILE
    edges = [(K + at, min(wide, size - at)) for at in range(0, size, wide)]

    def step(k, carry):
        k0 = pl.multiple_of(k * wide, wide)
        d0, d1 = pl.ds(k0, TILE), pl.ds(pl.multiple_of(k0 + TILE, TILE), TILE)
        dd = pl.ds(k0, wide)
        i0 = invert_tile(m_ref[d0, d0])
        b = m_ref[d0, d1]
        ct = m_ref[d1, d0]
        t = dot(i0, b)
        v = dot(ct, i0)
        i1 = invert_tile(m_ref[d1, d1] - dot(ct, t))
        ti = dot(t, i1)
        e = split3(
            jnp.concatenate(
                [
                    jnp.concatenate([i0 + dot(ti, v), -ti], axis=1),
                    jnp.concatenate([-dot(i1, v), i1], axis=1),
                ],
                axis=0,
            )
        )

        def scale(cs):
            h, m, l = split3(six(e, split3(m_ref[dd, cs])))
            gh[:, cs] = h
            gm[:, cs] = m
            gl[:, cs] = l

        def scale_pivot(j, carry):
            scale(pl.ds(pl.multiple_of(j * wide, wide), wide))
            return carry

        lax.fori_loop(k + 1, K // wide, scale_pivot, 0)
        for at, width in edges:
            scale(slice(at, at + width))

        def update(i, carry):
            ri = pl.ds(pl.multiple_of(i * TILE, TILE), TILE)
            left = split3(m_ref[ri, dd])

            def one(cs):
                m_ref[ri, cs] = m_ref[ri, cs] - six(left, (gh[:, cs], gm[:, cs], gl[:, cs]))

            def one_pivot(j, carry):
                one(pl.ds(pl.multiple_of(j * wide, wide), wide))
                return carry

            lax.fori_loop(k + 1, K // wide, one_pivot, 0)
            for at, width in edges:
                one(slice(at, at + width))
            return carry

        lax.fori_loop(2 * (k + 1), (K + size) // TILE, update, 0)
        return carry

    lax.fori_loop(0, K // wide, step, 0)
    out_ref[...] = m_ref[border, border]


def eliminate(idx, own, oth, mine, theirs, panel, factor):
    size = factor.shape[0]
    vmem = pl.BlockSpec(memory_space=pltpu.VMEM)
    return pl.pallas_call(
        schur_kernel,
        out_shape=jax.ShapeDtypeStruct(factor.shape, jnp.float32),
        in_specs=[pl.BlockSpec(memory_space=pltpu.SMEM)] + [vmem] * 6,
        out_specs=vmem,
        scratch_shapes=[pltpu.VMEM((K + size, K + size), jnp.float32)]
        + [pltpu.VMEM((2 * TILE, K + size), jnp.bfloat16)] * 3,
        name="eliminate",
    )(idx, own, oth, mine, theirs, panel, factor)


def z_pairs(d):
    return [(r, (r // 2 + d) % NZ * 2 + r % 2) for r in range(2 * NZ)]


def y_pairs(d):
    return [(c, (c // NX + d) % NY * NX + c % NX) for c in range(NX * NY)]


def x_pairs(d):
    return [(c, c // NX * NX + (c % NX + d) % NX) for c in range(NX * NY)]


FLIP = [(r, r ^ 1) for r in range(2 * NZ)]


def along_z(v, d):
    return lax.ppermute(v, "row", z_pairs(d))


def along_y(v, d):
    return lax.ppermute(v, "col", y_pairs(d))


def along_x(v, d):
    return lax.ppermute(v, "col", x_pairs(d))


together = lax.optimization_barrier


def pick(which, slots):
    return lax.select_n(which, *slots)


def per_device(factor):
    row_place = lax.axis_index("row")
    col_place = lax.axis_index("col")
    z, q = row_place // 2, row_place % 2
    y, x = col_place // NX, col_place % NX
    rows0 = factor[:TILE, :]
    cols0 = factor[:, :TILE]

    up1, down1 = along_z(rows0, 1), along_z(rows0, -1)
    pu1, pd1 = along_y(cols0, 1), along_y(cols0, -1)
    up1, down1, pu1, pd1 = together((up1, down1, pu1, pd1))
    up2, down2 = along_z(up1, 1), along_z(down1, -1)
    pu2 = along_y(pu1, 1)
    up2, down2, pu2 = together((up2, down2, pu2))
    pair = jnp.stack([pick(lax.rem(y - s + NY, NY), [cols0, pu1, pu2, pd1]) for s in range(2)])
    up3, down3 = along_z(up2, 1), along_z(down2, -1)
    xu, xd = along_x(pair, 1), along_x(pair, -1)
    up3, down3 = together((up3, down3))
    up4 = along_z(up3, 1)
    slots = [rows0, up1, up2, up3, up4, down3, down2, down1]
    mine = jnp.stack([pick(lax.rem(z - s + NZ, NZ), slots) for s in range(4)])
    mine, xu, xd = together((mine, xu, xd))
    part = mine[:, :, :TILE]
    au1, ad1 = along_y(part, 1), along_y(part, -1)
    far0, far1 = along_x(xu[0], 1), along_x(xd[1], -1)
    au1, ad1 = together((au1, ad1))
    au2 = along_y(au1, 1)
    theirs = lax.ppermute(mine, "row", FLIP)
    apair = jnp.stack([pick(lax.rem(y - s + NY, NY), [part, au1, au2, ad1]) for s in range(2)])
    apair, far0, far1 = together((apair, far0, far1))
    axu, axd = along_x(apair, 1), along_x(apair, -1)
    axu, axd, theirs = together((axu, axd, theirs))
    afar0, afar1 = along_x(axu[0], 1), along_x(axd[1], -1)
    own = jnp.stack([apair, axu, jnp.stack([afar0, afar1]), axd])
    other = lax.ppermute(own, "row", FLIP)
    panel = jnp.stack([pair, xu, jnp.stack([far0, far1]), xd])

    idx = jnp.stack([q, x, row_place, col_place]).astype(jnp.int32)
    return eliminate(idx, own, other, mine, theirs, panel, factor)


def solution(mesh):
    placed = (P("row", "col"),)
    return jax.shard_map(per_device, mesh=mesh, in_specs=placed, out_specs=P("row", "col"), check_vma=False)
```

```python
import jax
import jax.numpy as jnp
from jax import lax
from jax.experimental import pallas as pl
from jax.experimental.pallas import tpu as pltpu
from jax.sharding import PartitionSpec as P

TILE = 128
PIVOT = 512
STEPS = 2
K = PIVOT * STEPS
KT = K // TILE
HI = lax.Precision.HIGHEST
NZ, NY, NX = 8, 4, 4


def dot(a, b):
    return jnp.dot(a, b, precision=HI, preferred_element_type=jnp.float32)


def spread(x, e):
    return jnp.broadcast_to(x[e : e + 1, :], x.shape)


def invert_tile(block, b=16):
    n = TILE
    nb = b // 8
    nt = n // 8
    a = [block[8 * t : 8 * t + 8, :] for t in range(nt)]
    lane = lax.broadcasted_iota(jnp.int32, (8, n), 1)
    row = lax.broadcasted_iota(jnp.int32, (8, n), 0)
    for s in range(n // b):
        base = b * s
        own = [nb * s + q for q in range(nb)]
        inside = (lane >= base) & (lane < base + b)

        def col(t, j):
            return jnp.broadcast_to(a[t][:, base + j : base + j + 1], (8, n))

        c = [[col(t, j) for t in own] for j in range(b)]
        rows = [a[t] for t in own]
        for i in range(0, b, 2):
            h, e = divmod(i, 8)
            p, q_, w, o_ = spread(c[i][h], e), spread(c[i + 1][h], e), spread(c[i + 1][h], e + 1), spread(c[i][h], e + 1)
            rd = 1.0 / (p * w - q_ * o_)
            r0, r1 = row == e, row == e + 1
            l0, l1 = lane == base + i, lane == base + i + 1
            for j in range(i + 2, b):
                x, y = spread(c[j][h], e), spread(c[j][h], e + 1)
                u = (w * x - q_ * y) * rd
                v = (p * y - o_ * x) * rd
                for q in range(nb):
                    new = c[j][q] - c[i][q] * u - c[i + 1][q] * v
                    c[j][q] = jnp.where(r0, u, jnp.where(r1, v, new)) if q == h else new
            x = jnp.where(l0, 1.0, jnp.where(l1, 0.0, spread(rows[h], e)))
            y = jnp.where(l0, 0.0, jnp.where(l1, 1.0, spread(rows[h], e + 1)))
            u = (w * x - q_ * y) * rd
            v = (p * y - o_ * x) * rd
            for q in range(nb):
                new = jnp.where(l0 | l1, 0.0, rows[q]) - c[i][q] * u - c[i + 1][q] * v
                rows[q] = jnp.where(r0, u, jnp.where(r1, v, new)) if q == h else new
        g = [spread(rows[i // 8], i % 8) for i in range(b)]
        nxt = [nb * (s + 1) + q for q in range(nb)] if s + 1 < n // b else []
        rest = [t for t in range(nt) if t not in own and t not in nxt]
        full = jnp.concatenate(a, axis=0)
        d = dot(full[:, base : base + b], jnp.concatenate(rows, axis=0))
        for t in nxt:
            acc = jnp.where(inside, 0.0, a[t])
            for i in range(b):
                acc = acc - col(t, i) * g[i]
            a[t] = acc
        for t in rest:
            a[t] = jnp.where(inside, 0.0, a[t]) - d[8 * t : 8 * t + 8, :]
        for q, t in enumerate(own):
            a[t] = rows[q]
    return jnp.concatenate(a, axis=0)


def split3(x):
    h = x.astype(jnp.bfloat16)
    r = x - h.astype(jnp.float32)
    m = r.astype(jnp.bfloat16)
    l = (r - m.astype(jnp.float32)).astype(jnp.bfloat16)
    return h, m, l


def bdot(a, b):
    return jnp.dot(a, b, preferred_element_type=jnp.float32)


def inverse_kernel(idx_ref, own_ref, oth_ref, a_ref, gh, gm, gl):
    q, x, yf, zf = idx_ref[0], idx_ref[1], idx_ref[2], idx_ref[3]
    for xs in range(NX):
        slot = lax.rem(x - xs + NX, NX)
        for ys in range(2):
            cols = slice((NX * ys + xs) * TILE, (NX * ys + xs + 1) * TILE)
            for s in range(KT // 2):
                mine = pl.ds(pl.multiple_of((2 * s + q) * TILE, TILE), TILE)
                other = pl.ds(pl.multiple_of((2 * s + 1 - q) * TILE, TILE), TILE)
                a_ref[mine, cols] = own_ref[slot, lax.bitwise_xor(ys, yf), lax.bitwise_xor(s, zf)]
                a_ref[other, cols] = oth_ref[slot, lax.bitwise_xor(ys, yf), lax.bitwise_xor(s, zf)]

    def step(k, carry):
        k0 = pl.multiple_of(k * 2 * TILE, 2 * TILE)
        d0, d1 = pl.ds(k0, TILE), pl.ds(pl.multiple_of(k0 + TILE, TILE), TILE)
        dd = pl.ds(k0, 2 * TILE)
        i0 = invert_tile(a_ref[d0, d0])
        b = a_ref[d0, d1]
        ct = a_ref[d1, d0]
        t = dot(i0, b)
        v = dot(ct, i0)
        i1 = invert_tile(a_ref[d1, d1] - dot(ct, t))
        ti = dot(t, i1)
        e = jnp.concatenate(
            [
                jnp.concatenate([i0 + dot(ti, v), -ti], axis=1),
                jnp.concatenate([-dot(i1, v), i1], axis=1),
            ],
            axis=0,
        )
        for half in range(2):
            cs = slice(half * K // 2, (half + 1) * K // 2)
            a_ref[dd, cs] = dot(e, a_ref[dd, cs])
        a_ref[dd, dd] = e
        h, m, l = split3(a_ref[dd, :])
        gh[...] = h
        gm[...] = m
        gl[...] = l

        def update(i, carry):
            @pl.when(lax.div(i, 2) != k)
            def _():
                ri = pl.ds(pl.multiple_of(i * TILE, TILE), TILE)
                lh, lm, ll = split3(a_ref[ri, dd])
                a_ref[ri, dd] = jnp.zeros((TILE, 2 * TILE), jnp.float32)
                for part in range(4):
                    cs = slice(part * K // 4, (part + 1) * K // 4)
                    low = bdot(lm, gm[:, cs]) + bdot(lh, gl[:, cs]) + bdot(ll, gh[:, cs])
                    mid = bdot(lh, gm[:, cs]) + bdot(lm, gh[:, cs])
                    a_ref[ri, cs] = a_ref[ri, cs] - (bdot(lh, gh[:, cs]) + (mid + low))

            return carry

        return lax.fori_loop(0, KT, update, carry)

    lax.fori_loop(0, K // (2 * TILE), step, 0)


def pivot_inverse(idx, own, oth):
    return pl.pallas_call(
        inverse_kernel,
        out_shape=jax.ShapeDtypeStruct((K, K), jnp.float32),
        in_specs=[
            pl.BlockSpec(memory_space=pltpu.SMEM),
            pl.BlockSpec(memory_space=pltpu.VMEM),
            pl.BlockSpec(memory_space=pltpu.VMEM),
        ],
        out_specs=pl.BlockSpec(memory_space=pltpu.VMEM),
        scratch_shapes=[pltpu.VMEM((2 * TILE, K), jnp.bfloat16)] * 3,
        cost_estimate=pl.CostEstimate(flops=24 * K**3, bytes_accessed=12 * K**2, transcendentals=0),
        name="pivot_inverse",
    )(idx, own, oth)


def on_z(f):
    return [(2 * z + q, 2 * f(z) + q) for z in range(NZ) for q in range(2) if f(z) is not None]


def on_y(f):
    return [(NX * y + x, NX * f(y) + x) for y in range(NY) for x in range(NX) if f(y) is not None]


def on_x(d):
    return [(NX * y + x, NX * y + (x + d) % NX) for y in range(NY) for x in range(NX)]


Z_MIRROR = on_z(lambda z: NZ - 1 - z if z < NZ // 2 else None)
Y_MIRROR = on_y(lambda y: NY - 1 - y if y < NY // 2 else None)
FLIP = [(r, r ^ 1) for r in range(2 * NZ)]
together = lax.optimization_barrier


def per_device(factor):
    row_place = lax.axis_index("row")
    col_place = lax.axis_index("col")
    z, q = row_place // 2, row_place % 2
    y, x = col_place // NX, col_place % NX
    zf = jnp.minimum(z, NZ - 1 - z)
    yf = jnp.minimum(y, NY - 1 - y)
    size = factor.shape[1]

    def z_root(v):
        return jnp.where(z < NZ // 2, v, lax.ppermute(v, "row", Z_MIRROR))

    def z_swap(v, bit):
        return lax.ppermute(v, "row", on_z(lambda z: z ^ bit))

    def y_pair(v):
        v = jnp.where(y < NY // 2, v, lax.ppermute(v, "col", Y_MIRROR))
        return jnp.stack([v, lax.ppermute(v, "col", on_y(lambda y: y ^ 1))])

    tile = z_root(factor[:TILE, :TILE])
    two = jnp.stack([tile, z_swap(tile, 1)])
    corner = jnp.concatenate([two, z_swap(two, 2)])
    panel = y_pair(factor[:, :TILE])
    corner, panel, strip = together((corner, panel, factor[:TILE, :]))
    strip = z_root(strip)
    strip = jnp.stack([strip, z_swap(strip, 1)])
    pair = y_pair(corner)
    up, down = lax.ppermute(pair, "col", on_x(1)), lax.ppermute(pair, "col", on_x(-1))
    far0, far1 = lax.ppermute(up[0], "col", on_x(1)), lax.ppermute(down[1], "col", on_x(-1))
    own = jnp.stack([pair, up, jnp.stack([far0, far1]), down])
    own, panel, strip = together((own, panel, strip))
    other = lax.ppermute(own, "row", FLIP)
    slots = [panel] + [lax.ppermute(panel, "col", on_x(d)) for d in (1, 2, 3)]
    strip2 = z_swap(strip, 2)

    idx = jnp.stack([q, x, yf, zf]).astype(jnp.int32)
    inverse = pivot_inverse(idx, own, other)
    inverse, slots, strip, strip2 = together((inverse, slots, strip, strip2))
    strip = jnp.concatenate([strip, strip2])

    theirs = lax.ppermute(strip, "row", FLIP)
    tiles = []
    for c in range(KT):
        from_x = lax.select_n(lax.rem(x - c % NX + NX, NX), *slots)
        tiles.append(jnp.where(yf == c // NX, from_x[0], from_x[1]))
    cols = jnp.concatenate(tiles, axis=1)
    near = jnp.arange(size) < TILE
    is_row = (row_place < KT) & near
    is_col = (col_place < KT) & near
    at_row = jnp.arange(size) + row_place * TILE
    at_col = jnp.arange(size) + col_place * TILE
    pivots = jnp.arange(K)
    cols = jnp.where(is_row[:, None], -(at_row[:, None] == pivots[None, :]).astype(jnp.float32), cols)
    reduced, theirs = together((dot(cols, inverse), theirs))

    def swap1(v):
        return jnp.stack([v[1], v[0], v[3], v[2]])

    def in_order(v):
        v = jnp.where(zf % 2 == 1, swap1(v), v)
        return jnp.where(zf // 2 == 1, jnp.concatenate([v[2:], v[:2]]), v)

    mine, theirs = in_order(strip), in_order(theirs)
    rows = jnp.stack([jnp.where(q == 0, mine, theirs), jnp.where(q == 0, theirs, mine)], axis=1).reshape(K, size)
    rows = jnp.where(is_col[None, :], (pivots[:, None] == at_col[None, :]).astype(jnp.float32), rows)
    base = jnp.where(is_row[:, None] | is_col[None, :], 0.0, factor)
    return base - dot(reduced, rows)


def solution(mesh):
    placed = (P("row", "col"),)
    return jax.shard_map(per_device, mesh=mesh, in_specs=placed, out_specs=P("row", "col"), check_vma=False)
```

```python
import jax
import jax.numpy as jnp
from jax import lax
from jax.experimental import pallas as pl
from jax.experimental.pallas import tpu as pltpu
from jax.sharding import PartitionSpec as P

TILE = 128
PIVOT = 512
STEPS = 2
K = PIVOT * STEPS
KT = K // TILE
HI = lax.Precision.HIGHEST
NZ, NY, NX = 8, 4, 4


def dot(a, b):
    return jnp.dot(a, b, precision=HI, preferred_element_type=jnp.float32)


def spread(x, e):
    return jnp.broadcast_to(x[e : e + 1, :], x.shape)


def invert_tile(block, between, b=16):
    n = TILE
    nb = b // 8
    nt = n // 8
    a = [block[8 * t : 8 * t + 8, :] for t in range(nt)]
    lane = lax.broadcasted_iota(jnp.int32, (8, n), 1)
    row = lax.broadcasted_iota(jnp.int32, (8, n), 0)
    for s in range(n // b):
        base = b * s
        own = [nb * s + q for q in range(nb)]
        inside = (lane >= base) & (lane < base + b)

        def col(t, j):
            return jnp.broadcast_to(a[t][:, base + j : base + j + 1], (8, n))

        c = [[col(t, j) for t in own] for j in range(b)]
        rows = [a[t] for t in own]
        for i in range(0, b, 2):
            h, e = divmod(i, 8)
            p, q_, w, o_ = spread(c[i][h], e), spread(c[i + 1][h], e), spread(c[i + 1][h], e + 1), spread(c[i][h], e + 1)
            rd = 1.0 / (p * w - q_ * o_)
            r0, r1 = row == e, row == e + 1
            l0, l1 = lane == base + i, lane == base + i + 1
            for j in range(i + 2, b):
                x, y = spread(c[j][h], e), spread(c[j][h], e + 1)
                u = (w * x - q_ * y) * rd
                v = (p * y - o_ * x) * rd
                for q in range(nb):
                    new = c[j][q] - c[i][q] * u - c[i + 1][q] * v
                    c[j][q] = jnp.where(r0, u, jnp.where(r1, v, new)) if q == h else new
            x = jnp.where(l0, 1.0, jnp.where(l1, 0.0, spread(rows[h], e)))
            y = jnp.where(l0, 0.0, jnp.where(l1, 1.0, spread(rows[h], e + 1)))
            u = (w * x - q_ * y) * rd
            v = (p * y - o_ * x) * rd
            for q in range(nb):
                new = jnp.where(l0 | l1, 0.0, rows[q]) - c[i][q] * u - c[i + 1][q] * v
                rows[q] = jnp.where(r0, u, jnp.where(r1, v, new)) if q == h else new
        g = [spread(rows[i // 8], i % 8) for i in range(b)]
        nxt = [nb * (s + 1) + q for q in range(nb)] if s + 1 < n // b else []
        rest = [t for t in range(nt) if t not in own and t not in nxt]
        full = jnp.concatenate(a, axis=0)
        d = dot(full[:, base : base + b], jnp.concatenate(rows, axis=0))
        for t in nxt:
            acc = jnp.where(inside, 0.0, a[t])
            for i in range(b):
                acc = acc - col(t, i) * g[i]
            a[t] = acc
        for t in rest:
            a[t] = jnp.where(inside, 0.0, a[t]) - d[8 * t : 8 * t + 8, :]
        for q, t in enumerate(own):
            a[t] = rows[q]
        between()
    return jnp.concatenate(a, axis=0)


def split3(x):
    h = x.astype(jnp.bfloat16)
    r = x - h.astype(jnp.float32)
    m = r.astype(jnp.bfloat16)
    l = (r - m.astype(jnp.float32)).astype(jnp.bfloat16)
    return h, m, l


def bdot(a, b):
    return jnp.dot(a, b, preferred_element_type=jnp.float32)


def six(l, r):
    low = bdot(l[1], r[1]) + bdot(l[0], r[2]) + bdot(l[2], r[0])
    return bdot(l[0], r[0]) + (bdot(l[0], r[1]) + bdot(l[1], r[0]) + low)


WIDE = 2 * TILE
BLOCKS = K // WIDE


def block_at(j, part=None):
    if part is None:
        return pl.ds(pl.multiple_of(j * WIDE, WIDE), WIDE)
    return pl.ds(pl.multiple_of(j * WIDE + part * TILE, TILE), TILE)


def inverse_kernel(idx_ref, own_ref, oth_ref, a_ref, diag_ref, g_ref, left_ref):
    q, x, yf, zf = idx_ref[0], idx_ref[1], idx_ref[2], idx_ref[3]
    for xs in range(NX):
        slot = lax.rem(x - xs + NX, NX)
        for ys in range(2):
            cols = slice((NX * ys + xs) * TILE, (NX * ys + xs + 1) * TILE)
            for s in range(KT // 2):
                mine = pl.ds(pl.multiple_of((2 * s + q) * TILE, TILE), TILE)
                other = pl.ds(pl.multiple_of((2 * s + 1 - q) * TILE, TILE), TILE)
                at = (slot, lax.bitwise_xor(ys, yf), lax.bitwise_xor(s, zf))
                a_ref[mine, cols] = own_ref[at]
                a_ref[other, cols] = oth_ref[at]
    diag_ref[...] = a_ref[:WIDE, :WIDE]
    g_ref[...] = jnp.zeros(g_ref.shape, jnp.bfloat16)

    def get(ref, *at):
        return tuple(ref[(i,) + at] for i in range(3))

    def put(ref, value, *at):
        for i, v in enumerate(split3(value)):
            ref[(i,) + at] = v

    def load_left(n, rows, pivot):
        put(left_ref, a_ref[rows, block_at(pivot)], n)

    def apply(n, rows, cols):
        a_ref[rows, cols] = a_ref[rows, cols] - six(get(left_ref, n), get(g_ref, slice(None), cols))

    def apply_pivot(n, rows, pivot, live):
        cols = block_at(pivot)
        kept = a_ref[rows, cols]
        if live is not True:
            kept = jnp.where(live, 0.0, kept)
        else:
            kept = jnp.zeros_like(kept)
        a_ref[rows, cols] = kept - six(get(left_ref, n), get(g_ref, slice(None), cols))

    def step(k, carry):
        prev, n1, n2 = lax.rem(k + 3, BLOCKS), lax.rem(k + 1, BLOCKS), lax.rem(k + 2, BLOCKS)
        pieces = []
        for n in range(6):
            rows = block_at((k, n1, n2)[n // 2], n % 2)

            def load(n=n, rows=rows):
                load_left(n, rows, prev)

            targets = [block_at(j) for j in ((n1, n2) if n < 2 else (k, n1, n2))]
            for m, cols in enumerate(targets):

                def run(n=n, rows=rows, cols=cols, m=m, load=load):
                    if m == 0:
                        load()
                    apply(n, rows, cols)

                pieces.append(run)
            pieces.append(lambda n=n, rows=rows: apply_pivot(n, rows, prev, k > 0))
        total, calls, done = len(pieces), [0], [0]

        def between():
            calls[0] += 1
            while done[0] < total * calls[0] // (2 * (TILE // 16)):
                pieces[done[0]]()
                done[0] += 1

        i0 = invert_tile(diag_ref[:TILE, :TILE], between)
        b = diag_ref[:TILE, TILE:]
        ct = diag_ref[TILE:, :TILE]
        t = dot(i0, b)
        v = dot(ct, i0)
        i1 = invert_tile(diag_ref[TILE:, TILE:] - dot(ct, t), between)
        ti = dot(t, i1)
        e = jnp.concatenate(
            [
                jnp.concatenate([i0 + dot(ti, v), -ti], axis=1),
                jnp.concatenate([-dot(i1, v), i1], axis=1),
            ],
            axis=0,
        )
        rows = block_at(k)
        es = split3(e)
        for j in (n1, n2, prev):
            cols = block_at(j)
            scaled = six(es, split3(a_ref[rows, cols]))
            a_ref[rows, cols] = scaled
            put(g_ref, scaled, slice(None), cols)
        a_ref[rows, rows] = e
        for i in range(3):
            g_ref[i, :, rows] = es[i]

        @pl.when(k < BLOCKS - 1)
        def _():
            cols = block_at(n1)
            right = get(g_ref, slice(None), cols)
            for part in range(2):
                here = block_at(n1, part)
                new = a_ref[here, cols] - six(split3(a_ref[here, rows]), right)
                a_ref[here, cols] = new
                diag_ref[part * TILE : (part + 1) * TILE, :] = new

        return carry

    lax.fori_loop(0, BLOCKS, step, 0)

    def finish(n, carry):
        rows = pl.ds(pl.multiple_of(n * TILE, TILE), TILE)
        load_left(0, rows, BLOCKS - 1)
        for j in range(BLOCKS - 1):
            apply(0, rows, slice(j * WIDE, (j + 1) * WIDE))
        apply_pivot(0, rows, BLOCKS - 1, True)
        return carry

    lax.fori_loop(0, 2 * (BLOCKS - 1), finish, 0)


def pivot_inverse(idx, own, oth):
    vmem = pl.BlockSpec(memory_space=pltpu.VMEM)
    return pl.pallas_call(
        inverse_kernel,
        out_shape=jax.ShapeDtypeStruct((K, K), jnp.float32),
        in_specs=[pl.BlockSpec(memory_space=pltpu.SMEM), vmem, vmem],
        out_specs=vmem,
        scratch_shapes=[
            pltpu.VMEM((WIDE, WIDE), jnp.float32),
            pltpu.VMEM((3, WIDE, K), jnp.bfloat16),
            pltpu.VMEM((3, 6, TILE, WIDE), jnp.bfloat16),
        ],
        cost_estimate=pl.CostEstimate(flops=24 * K**3, bytes_accessed=12 * K**2, transcendentals=0),
        name="pivot_inverse",
    )(idx, own, oth)


def on_z(f):
    return [(2 * z + q, 2 * f(z) + q) for z in range(NZ) for q in range(2) if f(z) is not None]


def on_y(f):
    return [(NX * y + x, NX * f(y) + x) for y in range(NY) for x in range(NX) if f(y) is not None]


def on_x(d):
    return [(NX * y + x, NX * y + (x + d) % NX) for y in range(NY) for x in range(NX)]


Z_MIRROR = on_z(lambda z: NZ - 1 - z if z < NZ // 2 else None)
Y_MIRROR = on_y(lambda y: NY - 1 - y if y < NY // 2 else None)
FLIP = [(r, r ^ 1) for r in range(2 * NZ)]
together = lax.optimization_barrier


def per_device(factor):
    row_place = lax.axis_index("row")
    col_place = lax.axis_index("col")
    z, q = row_place // 2, row_place % 2
    y, x = col_place // NX, col_place % NX
    zf = jnp.minimum(z, NZ - 1 - z)
    yf = jnp.minimum(y, NY - 1 - y)
    size = factor.shape[1]

    def z_root(v):
        return jnp.where(z < NZ // 2, v, lax.ppermute(v, "row", Z_MIRROR))

    def z_swap(v, bit):
        return lax.ppermute(v, "row", on_z(lambda z: z ^ bit))

    def y_pair(v):
        v = jnp.where(y < NY // 2, v, lax.ppermute(v, "col", Y_MIRROR))
        return jnp.stack([v, lax.ppermute(v, "col", on_y(lambda y: y ^ 1))])

    tile, first_cols = together((z_root(factor[:TILE, :TILE]), factor[:, :TILE]))
    two = jnp.stack([tile, z_swap(tile, 1)])
    corner = jnp.concatenate([two, z_swap(two, 2)])
    panel = y_pair(first_cols)
    corner, panel, strip = together((corner, panel, factor[:TILE, :]))
    strip = z_root(strip)
    strip = jnp.stack([strip, z_swap(strip, 1)])
    pair = y_pair(corner)
    up, down = lax.ppermute(pair, "col", on_x(1)), lax.ppermute(pair, "col", on_x(-1))
    far0, far1 = lax.ppermute(up[0], "col", on_x(1)), lax.ppermute(down[1], "col", on_x(-1))
    own = jnp.stack([pair, up, jnp.stack([far0, far1]), down])
    own, panel, strip = together((own, panel, strip))
    other = lax.ppermute(own, "row", FLIP)
    slots = [panel] + [lax.ppermute(panel, "col", on_x(d)) for d in (1, 2, 3)]
    strip2 = z_swap(strip, 2)

    idx = jnp.stack([q, x, yf, zf]).astype(jnp.int32)
    inverse = pivot_inverse(idx, own, other)
    inverse, slots, strip, strip2 = together((inverse, slots, strip, strip2))
    strip = jnp.concatenate([strip, strip2])

    theirs = lax.ppermute(strip, "row", FLIP)
    tiles = []
    for c in range(KT):
        from_x = lax.select_n(lax.rem(x - c % NX + NX, NX), *slots)
        tiles.append(jnp.where(yf == c // NX, from_x[0], from_x[1]))
    cols = jnp.concatenate(tiles, axis=1)
    near = jnp.arange(size) < TILE
    is_row = (row_place < KT) & near
    is_col = (col_place < KT) & near
    at_row = jnp.arange(size) + row_place * TILE
    at_col = jnp.arange(size) + col_place * TILE
    pivots = jnp.arange(K)
    cols = jnp.where(is_row[:, None], -(at_row[:, None] == pivots[None, :]).astype(jnp.float32), cols)
    reduced, theirs = together((dot(cols, inverse), theirs))

    def swap1(v):
        return jnp.stack([v[1], v[0], v[3], v[2]])

    def in_order(v):
        v = jnp.where(zf % 2 == 1, swap1(v), v)
        return jnp.where(zf // 2 == 1, jnp.concatenate([v[2:], v[:2]]), v)

    mine, theirs = in_order(strip), in_order(theirs)
    rows = jnp.stack([jnp.where(q == 0, mine, theirs), jnp.where(q == 0, theirs, mine)], axis=1).reshape(K, size)
    rows = jnp.where(is_col[None, :], (pivots[:, None] == at_col[None, :]).astype(jnp.float32), rows)
    base = jnp.where(is_row[:, None] | is_col[None, :], 0.0, factor)
    return base - dot(reduced, rows)


def solution(mesh):
    placed = (P("row", "col"),)
    return jax.shard_map(per_device, mesh=mesh, in_specs=placed, out_specs=P("row", "col"), check_vma=False)
```

```python
import jax
import jax.numpy as jnp
from jax import lax
from jax.experimental import pallas as pl
from jax.experimental.pallas import tpu as pltpu
from jax.sharding import PartitionSpec as P

TILE = 128
PIVOT = 512
STEPS = 2
K = PIVOT * STEPS
KT = K // TILE
HI = lax.Precision.HIGHEST
NZ, NY, NX = 8, 4, 4


def dot(a, b):
    return jnp.dot(a, b, precision=HI, preferred_element_type=jnp.float32)


def spread(x, e):
    return jnp.broadcast_to(x[e : e + 1, :], x.shape)


def invert_tile(block, between, b=16):
    n = TILE
    nb = b // 8
    nt = n // 8
    a = [block[8 * t : 8 * t + 8, :] for t in range(nt)]
    lane = lax.broadcasted_iota(jnp.int32, (8, n), 1)
    row = lax.broadcasted_iota(jnp.int32, (8, n), 0)
    for s in range(n // b):
        base = b * s
        own = [nb * s + q for q in range(nb)]
        inside = (lane >= base) & (lane < base + b)

        def col(t, j):
            return jnp.broadcast_to(a[t][:, base + j : base + j + 1], (8, n))

        c = [[col(t, j) for t in own] for j in range(b)]
        rows = [a[t] for t in own]
        for i in range(0, b, 2):
            h, e = divmod(i, 8)
            p, q_, w, o_ = spread(c[i][h], e), spread(c[i + 1][h], e), spread(c[i + 1][h], e + 1), spread(c[i][h], e + 1)
            rd = 1.0 / (p * w - q_ * o_)
            r0, r1 = row == e, row == e + 1
            l0, l1 = lane == base + i, lane == base + i + 1
            for j in range(i + 2, b):
                x, y = spread(c[j][h], e), spread(c[j][h], e + 1)
                u = (w * x - q_ * y) * rd
                v = (p * y - o_ * x) * rd
                for q in range(nb):
                    new = c[j][q] - c[i][q] * u - c[i + 1][q] * v
                    c[j][q] = jnp.where(r0, u, jnp.where(r1, v, new)) if q == h else new
            x = jnp.where(l0, 1.0, jnp.where(l1, 0.0, spread(rows[h], e)))
            y = jnp.where(l0, 0.0, jnp.where(l1, 1.0, spread(rows[h], e + 1)))
            u = (w * x - q_ * y) * rd
            v = (p * y - o_ * x) * rd
            for q in range(nb):
                new = jnp.where(l0 | l1, 0.0, rows[q]) - c[i][q] * u - c[i + 1][q] * v
                rows[q] = jnp.where(r0, u, jnp.where(r1, v, new)) if q == h else new
        g = [spread(rows[i // 8], i % 8) for i in range(b)]
        nxt = [nb * (s + 1) + q for q in range(nb)] if s + 1 < n // b else []
        rest = [t for t in range(nt) if t not in own and t not in nxt]
        full = jnp.concatenate(a, axis=0)
        d = dot(full[:, base : base + b], jnp.concatenate(rows, axis=0))
        for t in nxt:
            acc = jnp.where(inside, 0.0, a[t])
            for i in range(b):
                acc = acc - col(t, i) * g[i]
            a[t] = acc
        for t in rest:
            a[t] = jnp.where(inside, 0.0, a[t]) - d[8 * t : 8 * t + 8, :]
        for q, t in enumerate(own):
            a[t] = rows[q]
        between()
    return jnp.concatenate(a, axis=0)


def split3(x):
    h = x.astype(jnp.bfloat16)
    r = x - h.astype(jnp.float32)
    m = r.astype(jnp.bfloat16)
    l = (r - m.astype(jnp.float32)).astype(jnp.bfloat16)
    return h, m, l


def bdot(a, b):
    return jnp.dot(a, b, preferred_element_type=jnp.float32)


def six(l, r):
    low = bdot(l[1], r[1]) + bdot(l[0], r[2]) + bdot(l[2], r[0])
    return bdot(l[0], r[0]) + (bdot(l[0], r[1]) + bdot(l[1], r[0]) + low)


WIDE = 2 * TILE
BLOCKS = K // WIDE


def block_at(j, part=None):
    if part is None:
        return pl.ds(pl.multiple_of(j * WIDE, WIDE), WIDE)
    return pl.ds(pl.multiple_of(j * WIDE + part * TILE, TILE), TILE)


def inverse_kernel(idx_ref, own_ref, oth_ref, a_ref, diag_ref, g_ref, left_ref):
    q, x, yf, zf = idx_ref[0], idx_ref[1], idx_ref[2], idx_ref[3]
    for xs in range(NX):
        slot = lax.rem(x - xs + NX, NX)
        for ys in range(2):
            cols = slice((NX * ys + xs) * TILE, (NX * ys + xs + 1) * TILE)
            for s in range(KT // 2):
                mine = pl.ds(pl.multiple_of((2 * s + q) * TILE, TILE), TILE)
                other = pl.ds(pl.multiple_of((2 * s + 1 - q) * TILE, TILE), TILE)
                at = (slot, lax.bitwise_xor(ys, yf), lax.bitwise_xor(s, zf))
                a_ref[mine, cols] = own_ref[at]
                a_ref[other, cols] = oth_ref[at]
    diag_ref[...] = a_ref[:WIDE, :WIDE]
    g_ref[...] = jnp.zeros(g_ref.shape, jnp.bfloat16)

    def get(ref, *at):
        return tuple(ref[(i,) + at] for i in range(3))

    def put(ref, value, *at):
        for i, v in enumerate(split3(value)):
            ref[(i,) + at] = v

    def load_left(n, rows, pivot):
        put(left_ref, a_ref[rows, block_at(pivot)], n)

    def apply(n, rows, cols):
        a_ref[rows, cols] = a_ref[rows, cols] - six(get(left_ref, n), get(g_ref, slice(None), cols))

    def apply_pivot(n, rows, pivot, live):
        cols = block_at(pivot)
        kept = a_ref[rows, cols]
        if live is not True:
            kept = jnp.where(live, 0.0, kept)
        else:
            kept = jnp.zeros_like(kept)
        a_ref[rows, cols] = kept - six(get(left_ref, n), get(g_ref, slice(None), cols))

    def step(k, carry):
        prev, n1, n2 = lax.rem(k + 3, BLOCKS), lax.rem(k + 1, BLOCKS), lax.rem(k + 2, BLOCKS)
        pieces = []
        for n in range(6):
            rows = block_at((k, n1, n2)[n // 2], n % 2)

            def load(n=n, rows=rows):
                load_left(n, rows, prev)

            targets = [block_at(j) for j in ((n1, n2) if n < 2 else (k, n1, n2))]
            for m, cols in enumerate(targets):

                def run(n=n, rows=rows, cols=cols, m=m, load=load):
                    if m == 0:
                        load()
                    apply(n, rows, cols)

                pieces.append(run)
            pieces.append(lambda n=n, rows=rows: apply_pivot(n, rows, prev, k > 0))
        total, calls, done = len(pieces), [0], [0]

        def between():
            calls[0] += 1
            while done[0] < total * calls[0] // (2 * (TILE // 16)):
                pieces[done[0]]()
                done[0] += 1

        i0 = invert_tile(diag_ref[:TILE, :TILE], between)
        b = diag_ref[:TILE, TILE:]
        ct = diag_ref[TILE:, :TILE]
        t = dot(i0, b)
        v = dot(ct, i0)
        i1 = invert_tile(diag_ref[TILE:, TILE:] - dot(ct, t), between)
        ti = dot(t, i1)
        e = jnp.concatenate(
            [
                jnp.concatenate([i0 + dot(ti, v), -ti], axis=1),
                jnp.concatenate([-dot(i1, v), i1], axis=1),
            ],
            axis=0,
        )
        rows = block_at(k)
        es = split3(e)
        for j in (n1, n2, prev):
            cols = block_at(j)
            scaled = six(es, split3(a_ref[rows, cols]))
            a_ref[rows, cols] = scaled
            put(g_ref, scaled, slice(None), cols)
        a_ref[rows, rows] = e
        for i in range(3):
            g_ref[i, :, rows] = es[i]

        @pl.when(k < BLOCKS - 1)
        def _():
            cols = block_at(n1)
            right = get(g_ref, slice(None), cols)
            for part in range(2):
                here = block_at(n1, part)
                new = a_ref[here, cols] - six(split3(a_ref[here, rows]), right)
                a_ref[here, cols] = new
                diag_ref[part * TILE : (part + 1) * TILE, :] = new

        return carry

    lax.fori_loop(0, BLOCKS, step, 0)

    def finish(n, carry):
        rows = pl.ds(pl.multiple_of(n * TILE, TILE), TILE)
        load_left(0, rows, BLOCKS - 1)
        for j in range(BLOCKS - 1):
            apply(0, rows, slice(j * WIDE, (j + 1) * WIDE))
        apply_pivot(0, rows, BLOCKS - 1, True)
        return carry

    lax.fori_loop(0, 2 * (BLOCKS - 1), finish, 0)


def pivot_inverse(idx, own, oth):
    vmem = pl.BlockSpec(memory_space=pltpu.VMEM)
    return pl.pallas_call(
        inverse_kernel,
        out_shape=jax.ShapeDtypeStruct((K, K), jnp.float32),
        in_specs=[pl.BlockSpec(memory_space=pltpu.SMEM), vmem, vmem],
        out_specs=vmem,
        scratch_shapes=[
            pltpu.VMEM((WIDE, WIDE), jnp.float32),
            pltpu.VMEM((3, WIDE, K), jnp.bfloat16),
            pltpu.VMEM((3, 6, TILE, WIDE), jnp.bfloat16),
        ],
        cost_estimate=pl.CostEstimate(flops=24 * K**3, bytes_accessed=12 * K**2, transcendentals=0),
        name="pivot_inverse",
    )(idx, own, oth)


def on_z(f):
    return [(2 * z + q, 2 * f(z) + q) for z in range(NZ) for q in range(2) if f(z) is not None]


def on_y(f):
    return [(NX * y + x, NX * f(y) + x) for y in range(NY) for x in range(NX) if f(y) is not None]


def on_x(d):
    return [(NX * y + x, NX * y + (x + d) % NX) for y in range(NY) for x in range(NX)]


Z_MIRROR = on_z(lambda z: NZ - 1 - z if z < NZ // 2 else None)
Y_MIRROR = on_y(lambda y: NY - 1 - y if y < NY // 2 else None)
FLIP = [(r, r ^ 1) for r in range(2 * NZ)]
together = lax.optimization_barrier


def per_device(factor):
    row_place = lax.axis_index("row")
    col_place = lax.axis_index("col")
    z, q = row_place // 2, row_place % 2
    y, x = col_place // NX, col_place % NX
    zf = jnp.minimum(z, NZ - 1 - z)
    yf = jnp.minimum(y, NY - 1 - y)
    size = factor.shape[1]

    def z_root(v):
        return jnp.where(z < NZ // 2, v, lax.ppermute(v, "row", Z_MIRROR))

    def z_swap(v, bit):
        return lax.ppermute(v, "row", on_z(lambda z: z ^ bit))

    def y_pair(v):
        v = jnp.where(y < NY // 2, v, lax.ppermute(v, "col", Y_MIRROR))
        return jnp.stack([v, lax.ppermute(v, "col", on_y(lambda y: y ^ 1))])

    tile = z_root(factor[:TILE, :TILE])
    two = jnp.stack([tile, z_swap(tile, 1)])
    corner = jnp.concatenate([two, z_swap(two, 2)])
    panel = y_pair(factor[:, :TILE])
    corner, panel, strip = together((corner, panel, factor[:TILE, :]))
    strip = z_root(strip)
    strip = jnp.stack([strip, z_swap(strip, 1)])
    pair = y_pair(corner)
    up, down = lax.ppermute(pair, "col", on_x(1)), lax.ppermute(pair, "col", on_x(-1))
    far0, far1 = lax.ppermute(up[0], "col", on_x(1)), lax.ppermute(down[1], "col", on_x(-1))
    own = jnp.stack([pair, up, jnp.stack([far0, far1]), down])
    own, panel, strip = together((own, panel, strip))
    other = lax.ppermute(own, "row", FLIP)
    slots = [panel] + [lax.ppermute(panel, "col", on_x(d)) for d in (1, 2, 3)]
    strip2 = z_swap(strip, 2)

    idx = jnp.stack([q, x, yf, zf]).astype(jnp.int32)
    inverse = pivot_inverse(idx, own, other)
    inverse, slots, strip, strip2 = together((inverse, slots, strip, strip2))
    strip = jnp.concatenate([strip, strip2])

    theirs = lax.ppermute(strip, "row", FLIP)
    tiles = []
    for c in range(KT):
        from_x = lax.select_n(lax.rem(x - c % NX + NX, NX), *slots)
        tiles.append(jnp.where(yf == c // NX, from_x[0], from_x[1]))
    cols = jnp.concatenate(tiles, axis=1)
    near = jnp.arange(size) < TILE
    is_row = (row_place < KT) & near
    is_col = (col_place < KT) & near
    at_row = jnp.arange(size) + row_place * TILE
    at_col = jnp.arange(size) + col_place * TILE
    pivots = jnp.arange(K)
    cols = jnp.where(is_row[:, None], -(at_row[:, None] == pivots[None, :]).astype(jnp.float32), cols)
    reduced, theirs = together((dot(cols, inverse), theirs))

    def swap1(v):
        return jnp.stack([v[1], v[0], v[3], v[2]])

    def in_order(v):
        v = jnp.where(zf % 2 == 1, swap1(v), v)
        return jnp.where(zf // 2 == 1, jnp.concatenate([v[2:], v[:2]]), v)

    mine, theirs = in_order(strip), in_order(theirs)
    rows = jnp.stack([jnp.where(q == 0, mine, theirs), jnp.where(q == 0, theirs, mine)], axis=1).reshape(K, size)
    rows = jnp.where(is_col[None, :], (pivots[:, None] == at_col[None, :]).astype(jnp.float32), rows)
    base = jnp.where(is_row[:, None] | is_col[None, :], 0.0, factor)
    return base - dot(reduced, rows)


def solution(mesh):
    placed = (P("row", "col"),)
    return jax.shard_map(per_device, mesh=mesh, in_specs=placed, out_specs=P("row", "col"), check_vma=False)
```

```python
import jax
import jax.numpy as jnp
from jax import lax
from jax.experimental import pallas as pl
from jax.experimental.pallas import tpu as pltpu
from jax.sharding import PartitionSpec as P

TILE = 128
PIVOT = 512
STEPS = 2
K = PIVOT * STEPS
KT = K // TILE
HI = lax.Precision.HIGHEST
NZ, NY, NX = 8, 4, 4


def dot(a, b):
    return jnp.dot(a, b, precision=HI, preferred_element_type=jnp.float32)


def spread(x, e):
    return jnp.broadcast_to(x[e : e + 1, :], x.shape)


def invert_tile(block, between, b=16):
    n = TILE
    nb = b // 8
    nt = n // 8
    a = [block[8 * t : 8 * t + 8, :] for t in range(nt)]
    lane = lax.broadcasted_iota(jnp.int32, (8, n), 1)
    row = lax.broadcasted_iota(jnp.int32, (8, n), 0)
    for s in range(n // b):
        base = b * s
        own = [nb * s + q for q in range(nb)]
        inside = (lane >= base) & (lane < base + b)

        def col(t, j):
            return jnp.broadcast_to(a[t][:, base + j : base + j + 1], (8, n))

        c = [[col(t, j) for t in own] for j in range(b)]
        rows = [a[t] for t in own]
        for i in range(0, b, 2):
            h, e = divmod(i, 8)
            p, q_, w, o_ = spread(c[i][h], e), spread(c[i + 1][h], e), spread(c[i + 1][h], e + 1), spread(c[i][h], e + 1)
            rd = 1.0 / (p * w - q_ * o_)
            r0, r1 = row == e, row == e + 1
            l0, l1 = lane == base + i, lane == base + i + 1
            for j in range(i + 2, b):
                x, y = spread(c[j][h], e), spread(c[j][h], e + 1)
                u = (w * x - q_ * y) * rd
                v = (p * y - o_ * x) * rd
                for q in range(nb):
                    new = c[j][q] - c[i][q] * u - c[i + 1][q] * v
                    c[j][q] = jnp.where(r0, u, jnp.where(r1, v, new)) if q == h else new
            x = jnp.where(l0, 1.0, jnp.where(l1, 0.0, spread(rows[h], e)))
            y = jnp.where(l0, 0.0, jnp.where(l1, 1.0, spread(rows[h], e + 1)))
            u = (w * x - q_ * y) * rd
            v = (p * y - o_ * x) * rd
            for q in range(nb):
                new = jnp.where(l0 | l1, 0.0, rows[q]) - c[i][q] * u - c[i + 1][q] * v
                rows[q] = jnp.where(r0, u, jnp.where(r1, v, new)) if q == h else new
        g = [spread(rows[i // 8], i % 8) for i in range(b)]
        nxt = [nb * (s + 1) + q for q in range(nb)] if s + 1 < n // b else []
        rest = [t for t in range(nt) if t not in own and t not in nxt]
        full = jnp.concatenate(a, axis=0)
        d = dot(full[:, base : base + b], jnp.concatenate(rows, axis=0))
        for t in nxt:
            acc = jnp.where(inside, 0.0, a[t])
            for i in range(b):
                acc = acc - col(t, i) * g[i]
            a[t] = acc
        for t in rest:
            a[t] = jnp.where(inside, 0.0, a[t]) - d[8 * t : 8 * t + 8, :]
        for q, t in enumerate(own):
            a[t] = rows[q]
        between()
    return jnp.concatenate(a, axis=0)


def split3(x):
    h = x.astype(jnp.bfloat16)
    r = x - h.astype(jnp.float32)
    m = r.astype(jnp.bfloat16)
    l = (r - m.astype(jnp.float32)).astype(jnp.bfloat16)
    return h, m, l


def bdot(a, b):
    return jnp.dot(a, b, preferred_element_type=jnp.float32)


def six(l, r):
    low = bdot(l[1], r[1]) + bdot(l[0], r[2]) + bdot(l[2], r[0])
    return bdot(l[0], r[0]) + (bdot(l[0], r[1]) + bdot(l[1], r[0]) + low)


WIDE = 2 * TILE
BLOCKS = K // WIDE


def block_at(j, part=None):
    if part is None:
        return pl.ds(pl.multiple_of(j * WIDE, WIDE), WIDE)
    return pl.ds(pl.multiple_of(j * WIDE + part * TILE, TILE), TILE)


def inverse_kernel(idx_ref, own_ref, oth_ref, a_ref, diag_ref, g_ref, left_ref):
    q, x, yf, zf = idx_ref[0], idx_ref[1], idx_ref[2], idx_ref[3]
    for xs in range(NX):
        slot = lax.rem(x - xs + NX, NX)
        for ys in range(2):
            cols = slice((NX * ys + xs) * TILE, (NX * ys + xs + 1) * TILE)
            for s in range(KT // 2):
                mine = pl.ds(pl.multiple_of((2 * s + q) * TILE, TILE), TILE)
                other = pl.ds(pl.multiple_of((2 * s + 1 - q) * TILE, TILE), TILE)
                at = (slot, lax.bitwise_xor(ys, yf), lax.bitwise_xor(s, zf))
                a_ref[mine, cols] = own_ref[at]
                a_ref[other, cols] = oth_ref[at]
    diag_ref[...] = a_ref[:WIDE, :WIDE]
    g_ref[...] = jnp.zeros(g_ref.shape, jnp.bfloat16)

    def get(ref, *at):
        return tuple(ref[(i,) + at] for i in range(3))

    def put(ref, value, *at):
        for i, v in enumerate(split3(value)):
            ref[(i,) + at] = v

    def load_left(n, rows, pivot):
        put(left_ref, a_ref[rows, block_at(pivot)], n)

    def apply(n, rows, cols):
        a_ref[rows, cols] = a_ref[rows, cols] - six(get(left_ref, n), get(g_ref, slice(None), cols))

    def apply_pivot(n, rows, pivot, live):
        cols = block_at(pivot)
        kept = a_ref[rows, cols]
        if live is not True:
            kept = jnp.where(live, 0.0, kept)
        else:
            kept = jnp.zeros_like(kept)
        a_ref[rows, cols] = kept - six(get(left_ref, n), get(g_ref, slice(None), cols))

    def step(k, carry):
        prev, n1, n2 = lax.rem(k + 3, BLOCKS), lax.rem(k + 1, BLOCKS), lax.rem(k + 2, BLOCKS)
        pieces = []
        for n in range(6):
            rows = block_at((k, n1, n2)[n // 2], n % 2)

            def load(n=n, rows=rows):
                load_left(n, rows, prev)

            targets = [block_at(j) for j in ((n1, n2) if n < 2 else (k, n1, n2))]
            for m, cols in enumerate(targets):

                def run(n=n, rows=rows, cols=cols, m=m, load=load):
                    if m == 0:
                        load()
                    apply(n, rows, cols)

                pieces.append(run)
            pieces.append(lambda n=n, rows=rows: apply_pivot(n, rows, prev, k > 0))
        total, calls, done = len(pieces), [0], [0]

        def between():
            calls[0] += 1
            while done[0] < total * calls[0] // (2 * (TILE // 16)):
                pieces[done[0]]()
                done[0] += 1

        i0 = invert_tile(diag_ref[:TILE, :TILE], between)
        b = diag_ref[:TILE, TILE:]
        ct = diag_ref[TILE:, :TILE]
        t = dot(i0, b)
        v = dot(ct, i0)
        i1 = invert_tile(diag_ref[TILE:, TILE:] - dot(ct, t), between)
        ti = dot(t, i1)
        e = jnp.concatenate(
            [
                jnp.concatenate([i0 + dot(ti, v), -ti], axis=1),
                jnp.concatenate([-dot(i1, v), i1], axis=1),
            ],
            axis=0,
        )
        rows = block_at(k)
        es = split3(e)
        for j in (n1, n2, prev):
            cols = block_at(j)
            scaled = six(es, split3(a_ref[rows, cols]))
            a_ref[rows, cols] = scaled
            put(g_ref, scaled, slice(None), cols)
        a_ref[rows, rows] = e
        for i in range(3):
            g_ref[i, :, rows] = es[i]

        @pl.when(k < BLOCKS - 1)
        def _():
            cols = block_at(n1)
            right = get(g_ref, slice(None), cols)
            for part in range(2):
                here = block_at(n1, part)
                new = a_ref[here, cols] - six(split3(a_ref[here, rows]), right)
                a_ref[here, cols] = new
                diag_ref[part * TILE : (part + 1) * TILE, :] = new

        return carry

    lax.fori_loop(0, BLOCKS, step, 0)

    def finish(n, carry):
        rows = pl.ds(pl.multiple_of(n * TILE, TILE), TILE)
        load_left(0, rows, BLOCKS - 1)
        for j in range(BLOCKS - 1):
            apply(0, rows, slice(j * WIDE, (j + 1) * WIDE))
        apply_pivot(0, rows, BLOCKS - 1, True)
        return carry

    lax.fori_loop(0, 2 * (BLOCKS - 1), finish, 0)


def pivot_inverse(idx, own, oth):
    vmem = pl.BlockSpec(memory_space=pltpu.VMEM)
    return pl.pallas_call(
        inverse_kernel,
        out_shape=jax.ShapeDtypeStruct((K, K), jnp.float32),
        in_specs=[pl.BlockSpec(memory_space=pltpu.SMEM), vmem, vmem],
        out_specs=vmem,
        scratch_shapes=[
            pltpu.VMEM((WIDE, WIDE), jnp.float32),
            pltpu.VMEM((3, WIDE, K), jnp.bfloat16),
            pltpu.VMEM((3, 6, TILE, WIDE), jnp.bfloat16),
        ],
        cost_estimate=pl.CostEstimate(flops=24 * K**3, bytes_accessed=12 * K**2, transcendentals=0),
        name="pivot_inverse",
    )(idx, own, oth)


def product_kernel(left_ref, right_ref, base_ref, out_ref, split_ref):
    deep = right_ref.shape[0]

    @pl.when(pl.program_id(0) == 0)
    def _():
        def split_rows(n, carry):
            rows = pl.ds(pl.multiple_of(n * TILE, TILE), TILE)
            for i, v in enumerate(split3(right_ref[rows, :])):
                split_ref[i, rows, :] = v
            return carry

        lax.fori_loop(0, deep // TILE, split_rows, 0)

    left = split3(left_ref[...])
    width = right_ref.shape[1]
    for at in range(0, width, WIDE):
        cols = slice(at, min(at + WIDE, width))
        out_ref[:, cols] = base_ref[:, cols] - six(left, tuple(split_ref[i, :, cols] for i in range(3)))


def minus_product(base, left, right):
    rows, deep = left.shape
    width = right.shape[1]
    return pl.pallas_call(
        product_kernel,
        grid=(rows // TILE,),
        out_shape=jax.ShapeDtypeStruct((rows, width), jnp.float32),
        in_specs=[
            pl.BlockSpec((TILE, deep), lambda i: (i, 0)),
            pl.BlockSpec((deep, width), lambda i: (0, 0)),
            pl.BlockSpec((TILE, width), lambda i: (i, 0)),
        ],
        out_specs=pl.BlockSpec((TILE, width), lambda i: (i, 0)),
        scratch_shapes=[pltpu.VMEM((3, deep, width), jnp.bfloat16)],
        cost_estimate=pl.CostEstimate(flops=12 * rows * deep * width, bytes_accessed=8 * deep * width, transcendentals=0),
        name="minus_product",
    )(left, right, base)


def on_z(f):
    return [(2 * z + q, 2 * f(z) + q) for z in range(NZ) for q in range(2) if f(z) is not None]


def on_y(f):
    return [(NX * y + x, NX * f(y) + x) for y in range(NY) for x in range(NX) if f(y) is not None]


def on_x(d):
    return [(NX * y + x, NX * y + (x + d) % NX) for y in range(NY) for x in range(NX)]


Z_MIRROR = on_z(lambda z: NZ - 1 - z if z < NZ // 2 else None)
Y_MIRROR = on_y(lambda y: NY - 1 - y if y < NY // 2 else None)
FLIP = [(r, r ^ 1) for r in range(2 * NZ)]
together = lax.optimization_barrier


def per_device(factor):
    row_place = lax.axis_index("row")
    col_place = lax.axis_index("col")
    z, q = row_place // 2, row_place % 2
    y, x = col_place // NX, col_place % NX
    zf = jnp.minimum(z, NZ - 1 - z)
    yf = jnp.minimum(y, NY - 1 - y)
    size = factor.shape[1]

    def z_root(v):
        return jnp.where(z < NZ // 2, v, lax.ppermute(v, "row", Z_MIRROR))

    def z_swap(v, bit):
        return lax.ppermute(v, "row", on_z(lambda z: z ^ bit))

    def y_pair(v):
        v = jnp.where(y < NY // 2, v, lax.ppermute(v, "col", Y_MIRROR))
        return jnp.stack([v, lax.ppermute(v, "col", on_y(lambda y: y ^ 1))])

    tile = z_root(factor[:TILE, :TILE])
    two = jnp.stack([tile, z_swap(tile, 1)])
    corner = jnp.concatenate([two, z_swap(two, 2)])
    panel = y_pair(factor[:, :TILE])
    corner, panel, strip = together((corner, panel, factor[:TILE, :]))
    strip = z_root(strip)
    strip = jnp.stack([strip, z_swap(strip, 1)])
    pair = y_pair(corner)
    up, down = lax.ppermute(pair, "col", on_x(1)), lax.ppermute(pair, "col", on_x(-1))
    far0, far1 = lax.ppermute(up[0], "col", on_x(1)), lax.ppermute(down[1], "col", on_x(-1))
    own = jnp.stack([pair, up, jnp.stack([far0, far1]), down])
    own, panel, strip = together((own, panel, strip))
    other = lax.ppermute(own, "row", FLIP)
    slots = [panel] + [lax.ppermute(panel, "col", on_x(d)) for d in (1, 2, 3)]
    strip2 = z_swap(strip, 2)

    idx = jnp.stack([q, x, yf, zf]).astype(jnp.int32)
    inverse = pivot_inverse(idx, own, other)
    inverse, slots, strip, strip2 = together((inverse, slots, strip, strip2))
    strip = jnp.concatenate([strip, strip2])

    theirs = lax.ppermute(strip, "row", FLIP)
    tiles = []
    for c in range(KT):
        from_x = lax.select_n(lax.rem(x - c % NX + NX, NX), *slots)
        tiles.append(jnp.where(yf == c // NX, from_x[0], from_x[1]))
    cols = jnp.concatenate(tiles, axis=1)
    near = jnp.arange(size) < TILE
    is_row = (row_place < KT) & near
    is_col = (col_place < KT) & near
    at_row = jnp.arange(size) + row_place * TILE
    at_col = jnp.arange(size) + col_place * TILE
    pivots = jnp.arange(K)
    cols = jnp.where(is_row[:, None], -(at_row[:, None] == pivots[None, :]).astype(jnp.float32), cols)
    reduced, theirs = together((dot(cols, inverse), theirs))

    def swap1(v):
        return jnp.stack([v[1], v[0], v[3], v[2]])

    def in_order(v):
        v = jnp.where(zf % 2 == 1, swap1(v), v)
        return jnp.where(zf // 2 == 1, jnp.concatenate([v[2:], v[:2]]), v)

    mine, theirs = in_order(strip), in_order(theirs)
    rows = jnp.stack([jnp.where(q == 0, mine, theirs), jnp.where(q == 0, theirs, mine)], axis=1).reshape(K, size)
    rows = jnp.where(is_col[None, :], (pivots[:, None] == at_col[None, :]).astype(jnp.float32), rows)
    base = jnp.where(is_row[:, None] | is_col[None, :], 0.0, factor)
    return minus_product(base, reduced, rows)


def solution(mesh):
    placed = (P("row", "col"),)
    return jax.shard_map(per_device, mesh=mesh, in_specs=placed, out_specs=P("row", "col"), check_vma=False)
```
